512 devices in a mesh: col: 64 (over y, z), inner: 2 (over core), outer: 4 (over x).
Axes of the slice: x: 4, y: 4, z: 16, core: 2. Of those that a mesh axis runs over, the one named last changes fastest.
Arguments:
- matrix: float32 [8192, 8192], P(('inner', 'outer'), 'col'), may hold values from -6 to 6
- sketch: float32 [8192, 256], P('col'), may hold values from -6 to 6
Outputs:
- basis: float32 [8192, 256], P(('inner', 'outer'))
- coeffs: float32 [256, 8192], P(None, 'col')
The draws below stay inside these ranges and needn't reach their ends.
All inputs are finite; a program needn't handle non-finite values.
Results may differ from the reference program's by a relative error of at most 0.0006.
Values sent between devices are 32-bit elements; how exact they have to be, the bound alone decides.
No kernel may reach another device: no remote copies, remote signals or barrier semaphores. Data moves between devices by JAX's collectives and lax.ppermute only.
A program may use at most 64 MiB of HBM per device.

```python
import jax
import jax.numpy as jnp
from jax import lax

M = 8192
K = 256
NCOL = 8192


def shard_levels(rng, extent, split, smallest, high):
    level, own = 1.0, jax.random.fold_in(rng, 6)
    for position, parts in split:
        steps = jnp.exp(jax.random.uniform(jax.random.fold_in(own, position), (parts,), jnp.float32, smallest / len(split), high / len(split)))
        level = level * jnp.repeat(steps, extent[position] // parts).reshape([-1 if axis == position else 1 for axis in range(len(extent))])
    return level


def scatter_about(own_key, shape, spread, bound, pieces=(), kind=jnp.bfloat16):
    result = jax.random.normal(own_key, shape, jnp.float32) * spread
    if len(pieces) > 0:
        result = shard_levels(own_key, shape, pieces, -0.22, 0.18) * result
    return jnp.clip(result, min=-bound, max=bound).astype(kind)


def setup_inputs(seed: int = 0) -> dict:
    key_list = jax.random.split(jax.random.key(seed), 3)
    return {
        "matrix": scatter_about(key_list[0], (M, NCOL), 1.0, 6.0, ((0, 8), (1, 64)), jnp.float32),
        "sketch": scatter_about(key_list[1], (NCOL, K), 1.0, 6.0, ((0, 64),), jnp.float32),
    }


def product(left, right):
    return jnp.dot(left.astype(jnp.float32), right.astype(jnp.float32), precision=lax.Precision.HIGHEST, preferred_element_type=jnp.float32)

def orthonormal(sample):
    factor_q, factor_r = jnp.linalg.qr(sample)
    signs = jnp.sign(jnp.diagonal(factor_r))
    return factor_q * signs[None, :]

def reference(matrix, sketch):
    basis_one = orthonormal(product(matrix, sketch))
    project_one = product(basis_one.T, matrix)
    basis_two = orthonormal(product(matrix, project_one.T))
    project_two = product(basis_two.T, matrix)
    scale = lax.rsqrt(lax.optimization_barrier(jnp.mean(project_two * project_two, axis=0, keepdims=True)) + 1e-06)
    return (basis_two * jnp.sqrt(jnp.float32(M)), project_two * scale)
```

```python
import jax
import jax.numpy as jnp
from jax import lax
from jax.sharding import Mesh, PartitionSpec as P

M = 8192
NEAR = ("y", "z_low")
FAR = "z_high"
ROWS = ("inner", "outer")


def dot(left, right, dims):
    return lax.dot_general(
        left,
        right,
        (dims, ((), ())),
        precision=lax.Precision.HIGHEST,
        preferred_element_type=jnp.float32,
    )


def scatter_sum(array, axis):
    tiles = array.reshape(lax.axis_size(axis), -1, array.shape[-1])
    return lax.all_to_all(tiles, axis, 0, 0, tiled=True).sum(axis=0)


def spread(array, axis):
    copies = jnp.broadcast_to(array[None], (lax.axis_size(axis), *array.shape))
    return lax.all_to_all(copies, axis, 0, 0, tiled=True)


def gather(array, axis):
    return spread(array, axis).reshape(-1, array.shape[-1])


def sum_over_columns(array):
    own = scatter_sum(scatter_sum(array, NEAR), FAR)
    return gather(gather(own, FAR), NEAR)


def sum_over_rows(array):
    return gather(scatter_sum(array, ROWS), ROWS)


def inverse_factor(gram):
    lower = jnp.linalg.cholesky(gram)
    identity = jnp.eye(gram.shape[0], dtype=gram.dtype)
    return jax.scipy.linalg.solve_triangular(lower, identity, lower=True)


def per_device(matrix, sketch):
    first = sum_over_columns(dot(matrix, sketch, ((1,), (0,))))
    transposed = spread(dot(matrix, first, ((0,), (0,))), ROWS).sum(axis=0)
    inverse_one = inverse_factor(sum_over_rows(dot(first, first, ((0,), (0,)))))
    product = sum_over_columns(dot(matrix, transposed, ((1,), (0,))))
    second = dot(product, inverse_one, ((1,), (1,)))
    gram = sum_over_rows(dot(second, second, ((0,), (0,))))
    coefficients = spread(dot(second, matrix, ((0,), (0,))), ROWS).sum(axis=0)
    inverse_two = inverse_factor(gram)
    basis = dot(second, inverse_two, ((1,), (1,)))
    projection = dot(inverse_two, coefficients, ((1,), (0,)))
    scale = lax.rsqrt(jnp.mean(projection * projection, axis=0, keepdims=True) + 1e-06)
    return (basis * jnp.sqrt(jnp.float32(M)), projection * scale)


def solution(mesh):
    columns, inner, outer = mesh.devices.shape
    split = Mesh(
        mesh.devices.reshape(4, columns // 8, 2, inner, outer),
        ("y", "z_high", "z_low", "inner", "outer"),
    )
    column = ("y", "z_high", "z_low")
    return jax.shard_map(
        per_device,
        mesh=split,
        in_specs=(P(ROWS, column), P(column, None)),
        out_specs=(P(ROWS, None), P(None, column)),
        check_vma=False,
    )
```

```python
import functools

import jax
import jax.numpy as jnp
from jax import lax
from jax.experimental import pallas as pl
from jax.experimental.pallas import tpu as pltpu
from jax.sharding import Mesh, PartitionSpec as P

M = 8192
NEAR = ("y", "z_low")
FAR = "z_high"
ROWS = ("inner", "outer")
STEP = 8
LANES = 128
BLOCK = 64


def dot(left, right, dims):
    return lax.dot_general(
        left,
        right,
        (dims, ((), ())),
        precision=lax.Precision.HIGHEST,
        preferred_element_type=jnp.float32,
    )


def factor_rows(tiles, first):
    depth = len(tiles)
    row = lax.broadcasted_iota(jnp.int32, (STEP, LANES), 0)
    roots = []
    for panel in range(depth):
        columns = []
        for i in range(STEP):
            tile, lane = divmod(first + panel * STEP + i, LANES)
            columns.append(
                [
                    jnp.broadcast_to(tiles[s][tile][:, lane : lane + 1], (STEP, LANES))
                    for s in range(panel, depth)
                ]
            )
        scale = jnp.zeros((STEP, LANES), jnp.float32)
        for i in range(STEP):
            root = lax.rsqrt(columns[i][0][i : i + 1, :])
            inverse = root * root
            scale = jnp.where(row == i, root, scale)
            weights = [column * inverse for column in columns[i]]
            weights[0] = jnp.where(row > i, weights[0], 0.0)
            for j in range(i + 1, STEP):
                partner = columns[i][0][j : j + 1, :]
                columns[j] = [c - w * partner for c, w in zip(columns[j], weights)]
            for t in range(len(tiles[panel])):
                source = tiles[panel][t][i : i + 1, :]
                for s in range(panel, depth):
                    tiles[s][t] = tiles[s][t] - weights[s - panel] * source
        roots.append(scale)
    return [[tile * roots[s] for tile in tiles[s]] for s in range(depth)]


def inverse_kernel(gram_ref, out_ref, work_ref):
    size = gram_ref.shape[0]
    rows = lax.broadcasted_iota(jnp.int32, (size, size), 0)
    lanes = lax.broadcasted_iota(jnp.int32, (size, size), 1)
    work_ref[:, :size] = gram_ref[...]
    work_ref[:, size:] = jnp.where(rows == lanes, 1.0, 0.0).astype(jnp.float32)
    for start in range(0, size, BLOCK):
        rest = start + BLOCK
        low = start // LANES * LANES
        high = size + -(-rest // LANES) * LANES
        tiles = [
            [
                work_ref[pl.ds(start + s, STEP), pl.ds(t, LANES)]
                for t in range(low, high, LANES)
            ]
            for s in range(0, BLOCK, STEP)
        ]
        tiles = factor_rows(tiles, start - low)
        whole = jnp.concatenate([jnp.concatenate(r, axis=1) for r in tiles], axis=0)
        out_ref[pl.ds(start, BLOCK), : high - size] = whole[:, size - low :]
        if high < 2 * size:
            out_ref[pl.ds(start, BLOCK), high - size :] = jnp.zeros(
                (BLOCK, 2 * size - high), jnp.float32
            )
        if rest < size:
            base = rest // LANES * LANES
            left = whole[:, base - low : size - low].T[rest - base :, :]
            work_ref[pl.ds(rest, size - rest), pl.ds(low, high - low)] -= dot(
                left, whole, ((1,), (0,))
            )


def inverse_factor(gram):
    size = gram.shape[0]
    return pl.pallas_call(
        inverse_kernel,
        out_shape=jax.ShapeDtypeStruct(gram.shape, jnp.float32),
        in_specs=[pl.BlockSpec(memory_space=pltpu.VMEM)],
        out_specs=pl.BlockSpec(memory_space=pltpu.VMEM),
        scratch_shapes=[pltpu.VMEM((size, 2 * size), jnp.float32)],
        cost_estimate=pl.CostEstimate(
            flops=2_000_000_000, transcendentals=size, bytes_accessed=8 * size * size
        ),
        name="inverse_factor",
    )(gram)


def exchange(tiles, axis):
    return lax.all_to_all(tiles, axis, 0, 0, tiled=True)


def tiles_for(array, axis):
    return array.reshape(lax.axis_size(axis), -1, array.shape[-1])


def copies_for(array, axis):
    return jnp.broadcast_to(array[None], (lax.axis_size(axis), *array.shape))


def scatter_sum(array, axis):
    return exchange(tiles_for(array, axis), axis).sum(axis=0)


def gather(array, axis):
    return exchange(copies_for(array, axis), axis).reshape(-1, array.shape[-1])


def sum_over_rows(array):
    return gather(scatter_sum(array, ROWS), ROWS)


def per_device(matrix, sketch):
    near = lax.axis_size(NEAR)
    rank = sketch.shape[1]
    width = matrix.shape[1]
    part = rank // near

    partial = dot(matrix, sketch, ((1,), (0,)))
    own = scatter_sum(scatter_sum(partial, NEAR), FAR)
    first = gather(gather(own, FAR), NEAR)

    own_gram = lax.dynamic_slice_in_dim(
        dot(first, first, ((0,), (0,))), lax.axis_index(NEAR) * part, part, 0
    )
    summed = sum_over_rows(
        jnp.concatenate([dot(matrix, first, ((0,), (0,))), own_gram], axis=0)
    )
    transposed, own_gram = summed[:width], summed[width:]

    partial = tiles_for(dot(matrix, transposed, ((1,), (0,))), NEAR)
    arrived = exchange(jnp.concatenate([partial, copies_for(own_gram, NEAR)], axis=1), NEAR)
    gram = arrived[:, -part:].reshape(rank, rank)
    own = scatter_sum(arrived[:, :-part].sum(axis=0), FAR)
    own = dot(own, inverse_factor(gram), ((1,), (1,)))
    second = gather(gather(own, FAR), NEAR)

    summed = sum_over_rows(
        jnp.concatenate(
            [dot(second, second, ((0,), (0,))), dot(matrix, second, ((0,), (0,)))], axis=0
        )
    )
    inverse = inverse_factor(summed[:rank])
    basis = dot(second, inverse, ((1,), (1,)))
    projection = dot(inverse, summed[rank:], ((1,), (1,)))
    scale = lax.rsqrt(jnp.mean(projection * projection, axis=0, keepdims=True) + 1e-06)
    return (basis * jnp.sqrt(jnp.float32(M)), projection * scale)


def solution(mesh):
    columns, inner, outer = mesh.devices.shape
    split = Mesh(
        mesh.devices.reshape(4, columns // 8, 2, inner, outer),
        ("y", "z_high", "z_low", "inner", "outer"),
    )
    column = ("y", "z_high", "z_low")
    return jax.shard_map(
        per_device,
        mesh=split,
        in_specs=(P(ROWS, column), P(column, None)),
        out_specs=(P(ROWS, None), P(None, column)),
        check_vma=False,
    )
```

```python
import jax
import jax.numpy as jnp
from jax import lax
from jax.experimental import pallas as pl
from jax.experimental.pallas import tpu as pltpu
from jax.sharding import Mesh, PartitionSpec as P

M = 8192
NEAR = ("y", "z_low")
FAR = "z_high"
ROWS = ("inner", "outer")
STEP = 8
LANES = 128
BLOCK = 32
PANEL = 2


def dot(left, right, dims):
    return lax.dot_general(
        left,
        right,
        (dims, ((), ())),
        precision=lax.Precision.HIGHEST,
        preferred_element_type=jnp.float32,
    )


def factor_rows(tiles, first):
    depth = len(tiles)
    row = lax.broadcasted_iota(jnp.int32, (STEP, LANES), 0)
    roots = []
    for panel in range(0, depth, PANEL):
        columns = []
        for i in range(STEP * PANEL):
            tile, lane = divmod(first + panel * STEP + i, LANES)
            columns.append(
                [
                    jnp.broadcast_to(tiles[s][tile][:, lane : lane + 1], (STEP, LANES))
                    for s in range(panel + i // STEP, depth)
                ]
            )
        scales = [jnp.zeros((STEP, LANES), jnp.float32) for _ in range(PANEL)]
        for i in range(STEP * PANEL):
            p, at = divmod(i, STEP)
            root = lax.rsqrt(columns[i][0][at : at + 1, :])
            inverse = root * root
            scales[p] = jnp.where(row == at, root, scales[p])
            weights = [column * inverse for column in columns[i]]
            weights[0] = jnp.where(row > at, weights[0], 0.0)
            for j in range(i + 1, STEP * PANEL):
                q, other = divmod(j, STEP)
                partner = columns[i][q - p][other : other + 1, :]
                columns[j] = [c - w * partner for c, w in zip(columns[j], weights[q - p :])]
            for t in range(len(tiles[panel])):
                source = tiles[panel + p][t][at : at + 1, :]
                for s in range(panel + p, depth):
                    tiles[s][t] = tiles[s][t] - weights[s - panel - p] * source
        roots += scales
    return [[tile * roots[s] for tile in tiles[s]] for s in range(depth)]


def invert_factor(gram, out_ref, work_ref):
    size = gram.shape[0]
    rows = lax.broadcasted_iota(jnp.int32, (size, size), 0)
    lanes = lax.broadcasted_iota(jnp.int32, (size, size), 1)
    work_ref[:, :size] = gram
    work_ref[:, size:] = jnp.where(rows == lanes, 1.0, 0.0).astype(jnp.float32)
    for start in range(0, size, BLOCK):
        rest = start + BLOCK
        low = start // LANES * LANES
        high = size + -(-rest // LANES) * LANES
        tiles = [
            [
                work_ref[pl.ds(start + s, STEP), pl.ds(t, LANES)]
                for t in range(low, high, LANES)
            ]
            for s in range(0, BLOCK, STEP)
        ]
        tiles = factor_rows(tiles, start - low)
        whole = jnp.concatenate([jnp.concatenate(r, axis=1) for r in tiles], axis=0)
        out_ref[pl.ds(start, BLOCK), : high - size] = whole[:, size - low :]
        if high < 2 * size:
            out_ref[pl.ds(start, BLOCK), high - size :] = jnp.zeros(
                (BLOCK, 2 * size - high), jnp.float32
            )
        if rest < size:
            base = rest // LANES * LANES
            left = whole[:, base - low : size - low].T[rest - base :, :]
            work_ref[pl.ds(rest, size - rest), pl.ds(low, high - low)] -= dot(
                left, whole, ((1,), (0,))
            )


def inverse_kernel(sums_ref, inverse_ref, work_ref):
    invert_factor(sums_ref[: inverse_ref.shape[0], :], inverse_ref, work_ref)


def projection_kernel(sums_ref, inverse_ref, coefficients_ref, work_ref):
    size = inverse_ref.shape[0]
    invert_factor(sums_ref[:size, :], inverse_ref, work_ref)
    projection = dot(inverse_ref[...], sums_ref[size:, :], ((1,), (1,)))
    mean = jnp.sum(projection * projection, axis=0, keepdims=True) / size
    coefficients_ref[...] = projection * lax.rsqrt(mean + 1e-06)


def on_sums(kernel, sums, others):
    rank = sums.shape[1]
    vmem = pl.BlockSpec(memory_space=pltpu.VMEM)
    shapes = [(rank, rank), *others]
    return pl.pallas_call(
        kernel,
        out_shape=[jax.ShapeDtypeStruct(shape, jnp.float32) for shape in shapes],
        in_specs=[vmem],
        out_specs=[vmem] * len(shapes),
        scratch_shapes=[pltpu.VMEM((rank, 2 * rank), jnp.float32)],
        cost_estimate=pl.CostEstimate(
            flops=2_000_000_000, transcendentals=rank, bytes_accessed=8 * rank * rank
        ),
        name=kernel.__name__,
    )(sums)


def exchange(tiles, axis):
    return lax.all_to_all(tiles, axis, 0, 0, tiled=True)


def tiles_for(array, axis):
    return array.reshape(lax.axis_size(axis), -1, array.shape[-1])


def copies_for(array, axis):
    return jnp.broadcast_to(array[None], (lax.axis_size(axis), *array.shape))


def scatter_sum(array, axis):
    return exchange(tiles_for(array, axis), axis).sum(axis=0)


def gather(array, axis):
    return exchange(copies_for(array, axis), axis).reshape(-1, array.shape[-1])


def sum_over_rows(array):
    return gather(scatter_sum(array, ROWS), ROWS)


def sums_with(matrix, sample):
    gram = dot(sample, sample, ((0,), (0,)))
    products = dot(matrix, sample, ((0,), (0,)))
    return sum_over_rows(jnp.concatenate([gram, products], axis=0))


def per_device(matrix, sketch):
    rank = sketch.shape[1]
    width = matrix.shape[1]

    partial = dot(matrix, sketch, ((1,), (0,)))
    own = scatter_sum(scatter_sum(partial, NEAR), FAR)
    first = gather(gather(own, FAR), NEAR)

    sums = sums_with(matrix, first)
    (inverse,) = on_sums(inverse_kernel, sums, [])
    partial = dot(matrix, sums[rank:], ((1,), (0,)))
    own = scatter_sum(scatter_sum(partial, NEAR), FAR)
    own = dot(own, inverse, ((1,), (1,)))
    second = gather(gather(own, FAR), NEAR)

    sums = sums_with(matrix, second)
    inverse, coefficients = on_sums(projection_kernel, sums, [(rank, width)])
    basis = dot(second, inverse, ((1,), (1,)))
    return (basis * jnp.sqrt(jnp.float32(M)), coefficients)


def solution(mesh):
    columns, inner, outer = mesh.devices.shape
    split = Mesh(
        mesh.devices.reshape(4, columns // 8, 2, inner, outer),
        ("y", "z_high", "z_low", "inner", "outer"),
    )
    column = ("y", "z_high", "z_low")
    return jax.shard_map(
        per_device,
        mesh=split,
        in_specs=(P(ROWS, column), P(column, None)),
        out_specs=(P(ROWS, None), P(None, column)),
        check_vma=False,
    )
```

```python
import jax
import jax.numpy as jnp
from jax import lax
from jax.experimental import pallas as pl
from jax.experimental.pallas import tpu as pltpu
from jax.sharding import Mesh, PartitionSpec as P

M = 8192
NEAR = ("y", "z_low")
FAR = "z_high"
ROWS = ("inner", "outer")
STEP = 8
LANES = 128
BLOCK = 32
PANEL = 2
CHUNKS = 4


def dot(left, right, dims):
    return lax.dot_general(
        left,
        right,
        (dims, ((), ())),
        precision=lax.Precision.HIGHEST,
        preferred_element_type=jnp.float32,
    )


def factor_rows(tiles, first):
    depth = len(tiles)
    row = lax.broadcasted_iota(jnp.int32, (STEP, LANES), 0)
    roots = []
    for panel in range(0, depth, PANEL):
        columns = []
        for i in range(STEP * PANEL):
            tile, lane = divmod(first + panel * STEP + i, LANES)
            columns.append(
                [
                    jnp.broadcast_to(tiles[s][tile][:, lane : lane + 1], (STEP, LANES))
                    for s in range(panel + i // STEP, depth)
                ]
            )
        scales = [jnp.zeros((STEP, LANES), jnp.float32) for _ in range(PANEL)]
        for i in range(STEP * PANEL):
            p, at = divmod(i, STEP)
            root = lax.rsqrt(columns[i][0][at : at + 1, :])
            inverse = root * root
            scales[p] = jnp.where(row == at, root, scales[p])
            weights = [column * inverse for column in columns[i]]
            weights[0] = jnp.where(row > at, weights[0], 0.0)
            for j in range(i + 1, STEP * PANEL):
                q, other = divmod(j, STEP)
                partner = columns[i][q - p][other : other + 1, :]
                columns[j] = [c - w * partner for c, w in zip(columns[j], weights[q - p :])]
            for t in range(len(tiles[panel])):
                source = tiles[panel + p][t][at : at + 1, :]
                for s in range(panel + p, depth):
                    tiles[s][t] = tiles[s][t] - weights[s - panel - p] * source
        roots += scales
    return [[tile * roots[s] for tile in tiles[s]] for s in range(depth)]


def invert_factor(sums_ref, out_ref, work_ref, between=None):
    size = out_ref.shape[0]
    half = size // 2
    rows = lax.broadcasted_iota(jnp.int32, (size, size), 0)
    lanes = lax.broadcasted_iota(jnp.int32, (size, size), 1)
    work_ref[half:, :size] = sums_ref[:half, :]
    work_ref[: half // 2, :half] = sums_ref[half : half + half // 2, :half]
    work_ref[half // 2 : half, :half] = sums_ref[half : half + half // 2, half:]
    work_ref[:half, half:size] = sums_ref[:half, :half].T
    work_ref[:, size:] = jnp.where(rows == lanes, 1.0, 0.0).astype(jnp.float32)
    for start in range(0, size, BLOCK):
        if between is not None:
            between(start)
        rest = start + BLOCK
        low = start // LANES * LANES
        high = size + -(-rest // LANES) * LANES
        tiles = [
            [
                work_ref[pl.ds(start + s, STEP), pl.ds(t, LANES)]
                for t in range(low, high, LANES)
            ]
            for s in range(0, BLOCK, STEP)
        ]
        tiles = factor_rows(tiles, start - low)
        whole = jnp.concatenate([jnp.concatenate(r, axis=1) for r in tiles], axis=0)
        out_ref[pl.ds(start, BLOCK), : high - size] = whole[:, size - low :]
        if high < 2 * size:
            out_ref[pl.ds(start, BLOCK), high - size :] = jnp.zeros(
                (BLOCK, 2 * size - high), jnp.float32
            )
        if rest < size:
            base = rest // LANES * LANES
            left = whole[:, base - low : size - low].T[rest - base :, :]
            work_ref[pl.ds(rest, size - rest), pl.ds(low, high - low)] -= dot(
                left, whole, ((1,), (0,))
            )


def result_kernel(
    sums_ref, sample_ref, basis_ref, coefficients_ref,
    inverse_ref, work_ref, left_ref, right_ref, in_sem, out_sems,
):
    size = inverse_ref.shape[0]
    half = size // 2
    count = sample_ref.shape[0]
    arriving = pltpu.make_async_copy(sample_ref, left_ref, in_sem)
    arriving.start()
    share = count // (half // BLOCK)

    def low_half(start):
        if start == half:
            arriving.wait()
        if start >= half:
            rows = pl.ds((start - half) // BLOCK * share, share)
            low = dot(left_ref[rows, :half], inverse_ref[:half, :half], ((1,), (1,)))
            right_ref[rows, :half] = low * M**0.5

    invert_factor(sums_ref, inverse_ref, work_ref, low_half)
    leaving = []
    for index, start in enumerate(range(0, count, count // CHUNKS)):
        part = pl.ds(start, count // CHUNKS)
        high = dot(left_ref[part, :], inverse_ref[half:, :], ((1,), (1,)))
        right_ref[part, half:] = high * M**0.5
        leaving.append(
            pltpu.make_async_copy(right_ref.at[part], basis_ref.at[part], out_sems.at[index])
        )
        leaving[-1].start()
    products = sums_ref[half + half // 2 :, :]
    projection = dot(inverse_ref[...], products, ((1,), (1,)))
    mean = jnp.sum(projection * projection, axis=0, keepdims=True) / size
    coefficients_ref[...] = projection * lax.rsqrt(mean + 1e-06)
    for copy in leaving:
        copy.wait()


def work_for(rank):
    return pltpu.VMEM((rank, 2 * rank), jnp.float32)


def price_of(rank):
    return pl.CostEstimate(
        flops=2_000_000_000, transcendentals=rank, bytes_accessed=8 * rank * rank
    )


def inverse_factor(sums):
    rank = sums.shape[1]
    vmem = pl.BlockSpec(memory_space=pltpu.VMEM)
    return pl.pallas_call(
        invert_factor,
        out_shape=jax.ShapeDtypeStruct((rank, rank), jnp.float32),
        in_specs=[vmem],
        out_specs=vmem,
        scratch_shapes=[work_for(rank)],
        cost_estimate=price_of(rank),
        name="inverse_factor",
    )(sums)


def results(sums, sample, width):
    rank = sums.shape[1]
    vmem = pl.BlockSpec(memory_space=pltpu.VMEM)
    anywhere = pl.BlockSpec(memory_space=pl.ANY)
    return pl.pallas_call(
        result_kernel,
        out_shape=[
            jax.ShapeDtypeStruct(sample.shape, jnp.float32),
            jax.ShapeDtypeStruct((rank, width), jnp.float32),
        ],
        in_specs=[vmem, anywhere],
        out_specs=[anywhere, vmem],
        scratch_shapes=[
            pltpu.VMEM((rank, rank), jnp.float32),
            work_for(rank),
            pltpu.VMEM(sample.shape, jnp.float32),
            pltpu.VMEM(sample.shape, jnp.float32),
            pltpu.SemaphoreType.DMA(()),
            pltpu.SemaphoreType.DMA((CHUNKS,)),
        ],
        cost_estimate=price_of(rank),
        name="results",
    )(sums, sample)


def exchange(tiles, axis):
    return lax.all_to_all(tiles, axis, 0, 0, tiled=True)


def tiles_for(array, axis):
    return array.reshape(lax.axis_size(axis), -1, array.shape[-1])


def copies_for(array, axis):
    return jnp.broadcast_to(array[None], (lax.axis_size(axis), *array.shape))


def scatter_sum(array, axis):
    return exchange(tiles_for(array, axis), axis).sum(axis=0)


def gather(array, axis):
    return exchange(copies_for(array, axis), axis).reshape(-1, array.shape[-1])


def sum_over_rows(array):
    return gather(scatter_sum(array, ROWS), ROWS)


def sums_with(matrix, sample):
    half = sample.shape[1] // 2
    lower = dot(sample[:, half:], sample, ((0,), (0,)))
    corner = dot(sample[:, :half], sample[:, :half], ((0,), (0,)))
    corner = jnp.concatenate([corner[: half // 2], corner[half // 2 :]], axis=1)
    products = dot(matrix, sample, ((0,), (0,)))
    return sum_over_rows(jnp.concatenate([lower, corner, products], axis=0))


def per_device(matrix, sketch):
    width = matrix.shape[1]

    partial = dot(matrix, sketch, ((1,), (0,)))
    own = scatter_sum(scatter_sum(partial, NEAR), FAR)
    first = gather(gather(own, FAR), NEAR)

    sums = sums_with(matrix, first)
    inverse = inverse_factor(sums)
    partial = dot(matrix, sums[-width:], ((1,), (0,)))
    own = scatter_sum(scatter_sum(partial, NEAR), FAR)
    own = dot(own, inverse, ((1,), (1,)))
    second = gather(gather(own, FAR), NEAR)

    return tuple(results(sums_with(matrix, second), second, width))


def solution(mesh):
    columns, inner, outer = mesh.devices.shape
    split = Mesh(
        mesh.devices.reshape(4, columns // 8, 2, inner, outer),
        ("y", "z_high", "z_low", "inner", "outer"),
    )
    column = ("y", "z_high", "z_low")
    return jax.shard_map(
        per_device,
        mesh=split,
        in_specs=(P(ROWS, column), P(column, None)),
        out_specs=(P(ROWS, None), P(None, column)),
        check_vma=False,
    )
```

```python
import jax
import jax.numpy as jnp
from jax import lax
from jax.experimental import pallas as pl
from jax.experimental.pallas import tpu as pltpu
from jax.sharding import Mesh, PartitionSpec as P

M = 8192
NEAR = ("z_low", "y")
FAR = "z_high"
ROWS = ("inner", "outer")
PEERS = ("outer", "inner")
STEP = 8
LANES = 128
BLOCK = 32
PANEL = 2
CHUNKS = 4


def dot(left, right, dims):
    return lax.dot_general(
        left,
        right,
        (dims, ((), ())),
        precision=lax.Precision.HIGHEST,
        preferred_element_type=jnp.float32,
    )


def factor_rows(tiles, first):
    depth = len(tiles)
    row = lax.broadcasted_iota(jnp.int32, (STEP, LANES), 0)
    roots = []
    for panel in range(0, depth, PANEL):
        columns = []
        for i in range(STEP * PANEL):
            tile, lane = divmod(first + panel * STEP + i, LANES)
            columns.append(
                [
                    jnp.broadcast_to(tiles[s][tile][:, lane : lane + 1], (STEP, LANES))
                    for s in range(panel + i // STEP, depth)
                ]
            )
        scales = [jnp.zeros((STEP, LANES), jnp.float32) for _ in range(PANEL)]
        for i in range(STEP * PANEL):
            p, at = divmod(i, STEP)
            root = lax.rsqrt(columns[i][0][at : at + 1, :])
            inverse = root * root
            scales[p] = jnp.where(row == at, root, scales[p])
            weights = [column * inverse for column in columns[i]]
            weights[0] = jnp.where(row > at, weights[0], 0.0)
            for j in range(i + 1, STEP * PANEL):
                q, other = divmod(j, STEP)
                partner = columns[i][q - p][other : other + 1, :]
                columns[j] = [c - w * partner for c, w in zip(columns[j], weights[q - p :])]
            for t in range(len(tiles[panel])):
                source = tiles[panel + p][t][at : at + 1, :]
                for s in range(panel + p, depth):
                    tiles[s][t] = tiles[s][t] - weights[s - panel - p] * source
        roots += scales
    return [[tile * roots[s] for tile in tiles[s]] for s in range(depth)]


def invert_factor(sums_ref, out_ref, work_ref, between=None):
    size = out_ref.shape[0]
    half = size // 2
    rows = lax.broadcasted_iota(jnp.int32, (size, size), 0)
    lanes = lax.broadcasted_iota(jnp.int32, (size, size), 1)
    work_ref[half:, :size] = sums_ref[:half, :]
    work_ref[: half // 2, :half] = sums_ref[half : half + half // 2, :half]
    work_ref[half // 2 : half, :half] = sums_ref[half : half + half // 2, half:]
    work_ref[:half, half:size] = sums_ref[:half, :half].T
    work_ref[:, size:] = jnp.where(rows == lanes, 1.0, 0.0).astype(jnp.float32)
    for start in range(0, size, BLOCK):
        if between is not None:
            between(start)
        rest = start + BLOCK
        low = start // LANES * LANES
        high = size + -(-rest // LANES) * LANES
        tiles = [
            [
                work_ref[pl.ds(start + s, STEP), pl.ds(t, LANES)]
                for t in range(low, high, LANES)
            ]
            for s in range(0, BLOCK, STEP)
        ]
        tiles = factor_rows(tiles, start - low)
        whole = jnp.concatenate([jnp.concatenate(r, axis=1) for r in tiles], axis=0)
        out_ref[pl.ds(start, BLOCK), : high - size] = whole[:, size - low :]
        if high < 2 * size:
            out_ref[pl.ds(start, BLOCK), high - size :] = jnp.zeros(
                (BLOCK, 2 * size - high), jnp.float32
            )
        if rest < size:
            base = rest // LANES * LANES
            left = whole[:, base - low : size - low].T[rest - base :, :]
            work_ref[pl.ds(rest, size - rest), pl.ds(low, high - low)] -= dot(
                left, whole, ((1,), (0,))
            )


def result_kernel(
    sums_ref, sample_ref, basis_ref, coefficients_ref,
    inverse_ref, work_ref, left_ref, right_ref, in_sem, out_sems,
):
    size = inverse_ref.shape[0]
    half = size // 2
    count = sample_ref.shape[0]
    arriving = pltpu.make_async_copy(sample_ref, left_ref, in_sem)
    arriving.start()
    share = count // (half // BLOCK)

    def low_half(start):
        if start == half:
            arriving.wait()
        if start >= half:
            rows = pl.ds((start - half) // BLOCK * share, share)
            low = dot(left_ref[rows, :half], inverse_ref[:half, :half], ((1,), (1,)))
            right_ref[rows, :half] = low * M**0.5

    invert_factor(sums_ref, inverse_ref, work_ref, low_half)
    leaving = []
    for index, start in enumerate(range(0, count, count // CHUNKS)):
        part = pl.ds(start, count // CHUNKS)
        high = dot(left_ref[part, :], inverse_ref[half:, :], ((1,), (1,)))
        right_ref[part, half:] = high * M**0.5
        leaving.append(
            pltpu.make_async_copy(right_ref.at[part], basis_ref.at[part], out_sems.at[index])
        )
        leaving[-1].start()
    products = sums_ref[half + half // 2 :, :]
    projection = dot(inverse_ref[...], products, ((1,), (1,)))
    mean = jnp.sum(projection * projection, axis=0, keepdims=True) / size
    coefficients_ref[...] = projection * lax.rsqrt(mean + 1e-06)
    for copy in leaving:
        copy.wait()


def work_for(rank):
    return pltpu.VMEM((rank, 2 * rank), jnp.float32)


def price_of(rank):
    return pl.CostEstimate(
        flops=2_000_000_000, transcendentals=rank, bytes_accessed=8 * rank * rank
    )


def inverse_factor(sums):
    rank = sums.shape[1]
    vmem = pl.BlockSpec(memory_space=pltpu.VMEM)
    return pl.pallas_call(
        invert_factor,
        out_shape=jax.ShapeDtypeStruct((rank, rank), jnp.float32),
        in_specs=[vmem],
        out_specs=vmem,
        scratch_shapes=[work_for(rank)],
        cost_estimate=price_of(rank),
        name="inverse_factor",
    )(sums)


def results(sums, sample, width):
    rank = sums.shape[1]
    vmem = pl.BlockSpec(memory_space=pltpu.VMEM)
    anywhere = pl.BlockSpec(memory_space=pl.ANY)
    return pl.pallas_call(
        result_kernel,
        out_shape=[
            jax.ShapeDtypeStruct(sample.shape, jnp.float32),
            jax.ShapeDtypeStruct((rank, width), jnp.float32),
        ],
        in_specs=[vmem, anywhere],
        out_specs=[anywhere, vmem],
        scratch_shapes=[
            pltpu.VMEM((rank, rank), jnp.float32),
            work_for(rank),
            pltpu.VMEM(sample.shape, jnp.float32),
            pltpu.VMEM(sample.shape, jnp.float32),
            pltpu.SemaphoreType.DMA(()),
            pltpu.SemaphoreType.DMA((CHUNKS,)),
        ],
        cost_estimate=price_of(rank),
        name="results",
    )(sums, sample)


def exchange(tiles, axis):
    return lax.all_to_all(tiles, axis, 0, 0, tiled=True)


def tiles_for(array, axis):
    return array.reshape(lax.axis_size(axis), -1, array.shape[-1])


def copies_for(array, axis):
    return jnp.broadcast_to(array[None], (lax.axis_size(axis), *array.shape))


def scatter_sum(array, axis):
    return exchange(tiles_for(array, axis), axis).sum(axis=0)


def gather(array, axis):
    return exchange(copies_for(array, axis), axis).reshape(-1, array.shape[-1])


def sum_over_rows(array):
    return gather(scatter_sum(array, PEERS), PEERS)


def sums_with(matrix, sample):
    half = sample.shape[1] // 2
    lower = dot(sample[:, half:], sample, ((0,), (0,)))
    corner = dot(sample[:, :half], sample[:, :half], ((0,), (0,)))
    corner = jnp.concatenate([corner[: half // 2], corner[half // 2 :]], axis=1)
    products = dot(matrix, sample, ((0,), (0,)))
    return sum_over_rows(jnp.concatenate([lower, corner, products], axis=0))


def per_device(matrix, sketch):
    width = matrix.shape[1]

    partial = dot(matrix, sketch, ((1,), (0,)))
    own = scatter_sum(scatter_sum(partial, NEAR), FAR)
    first = gather(gather(own, FAR), NEAR)

    sums = sums_with(matrix, first)
    inverse = inverse_factor(sums)
    partial = dot(matrix, sums[-width:], ((1,), (0,)))
    own = scatter_sum(scatter_sum(partial, NEAR), FAR)
    own = dot(own, inverse, ((1,), (1,)))
    second = gather(gather(own, FAR), NEAR)

    return tuple(results(sums_with(matrix, second), second, width))


def solution(mesh):
    columns, inner, outer = mesh.devices.shape
    split = Mesh(
        mesh.devices.reshape(4, columns // 8, 2, inner, outer),
        ("y", "z_high", "z_low", "inner", "outer"),
    )
    column = ("y", "z_high", "z_low")
    return jax.shard_map(
        per_device,
        mesh=split,
        in_specs=(P(ROWS, column), P(column, None)),
        out_specs=(P(ROWS, None), P(None, column)),
        check_vma=False,
    )
```

```python
import jax
import jax.numpy as jnp
from jax import lax
from jax.experimental import pallas as pl
from jax.experimental.pallas import tpu as pltpu
from jax.sharding import Mesh, PartitionSpec as P

M = 8192
NEAR = ("z_low", "y")
FAR = "z_high"
ROWS = ("inner", "outer")
STEP = 8
LANES = 128
BLOCK = 32
PANEL = 2
CHUNKS = 4


def dot(left, right, dims):
    return lax.dot_general(
        left,
        right,
        (dims, ((), ())),
        precision=lax.Precision.HIGHEST,
        preferred_element_type=jnp.float32,
    )


def factor_rows(tiles, first):
    depth = len(tiles)
    row = lax.broadcasted_iota(jnp.int32, (STEP, LANES), 0)
    roots = []
    for panel in range(0, depth, PANEL):
        columns = []
        for i in range(STEP * PANEL):
            tile, lane = divmod(first + panel * STEP + i, LANES)
            columns.append(
                [
                    jnp.broadcast_to(tiles[s][tile][:, lane : lane + 1], (STEP, LANES))
                    for s in range(panel + i // STEP, depth)
                ]
            )
        scales = [jnp.zeros((STEP, LANES), jnp.float32) for _ in range(PANEL)]
        for i in range(STEP * PANEL):
            p, at = divmod(i, STEP)
            root = lax.rsqrt(columns[i][0][at : at + 1, :])
            inverse = root * root
            scales[p] = jnp.where(row == at, root, scales[p])
            weights = [column * inverse for column in columns[i]]
            weights[0] = jnp.where(row > at, weights[0], 0.0)
            for j in range(i + 1, STEP * PANEL):
                q, other = divmod(j, STEP)
                partner = columns[i][q - p][other : other + 1, :]
                columns[j] = [c - w * partner for c, w in zip(columns[j], weights[q - p :])]
            for t in range(len(tiles[panel])):
                source = tiles[panel + p][t][at : at + 1, :]
                for s in range(panel + p, depth):
                    tiles[s][t] = tiles[s][t] - weights[s - panel - p] * source
        roots += scales
    return [[tile * roots[s] for tile in tiles[s]] for s in range(depth)]


def invert_factor(sums_ref, out_ref, work_ref, between=None):
    size = out_ref.shape[0]
    half = size // 2
    rows = lax.broadcasted_iota(jnp.int32, (size, size), 0)
    lanes = lax.broadcasted_iota(jnp.int32, (size, size), 1)
    work_ref[half:, :size] = sums_ref[:half, :]
    work_ref[: half // 2, :half] = sums_ref[half : half + half // 2, :half]
    work_ref[half // 2 : half, :half] = sums_ref[half : half + half // 2, half:]
    work_ref[:half, half:size] = sums_ref[:half, :half].T
    work_ref[:, size:] = jnp.where(rows == lanes, 1.0, 0.0).astype(jnp.float32)
    for start in range(0, size, BLOCK):
        if between is not None:
            between(start)
        rest = start + BLOCK
        low = start // LANES * LANES
        high = size + -(-rest // LANES) * LANES
        tiles = [
            [
                work_ref[pl.ds(start + s, STEP), pl.ds(t, LANES)]
                for t in range(low, high, LANES)
            ]
            for s in range(0, BLOCK, STEP)
        ]
        tiles = factor_rows(tiles, start - low)
        whole = jnp.concatenate([jnp.concatenate(r, axis=1) for r in tiles], axis=0)
        out_ref[pl.ds(start, BLOCK), : high - size] = whole[:, size - low :]
        if high < 2 * size:
            out_ref[pl.ds(start, BLOCK), high - size :] = jnp.zeros(
                (BLOCK, 2 * size - high), jnp.float32
            )
        if rest < size:
            base = rest // LANES * LANES
            left = whole[:, base - low : size - low].T[rest - base :, :]
            work_ref[pl.ds(rest, size - rest), pl.ds(low, high - low)] -= dot(
                left, whole, ((1,), (0,))
            )


def result_kernel(
    sums_ref, sample_ref, basis_ref, coefficients_ref,
    inverse_ref, work_ref, left_ref, right_ref, in_sem, out_sems,
):
    size = inverse_ref.shape[0]
    half = size // 2
    count = sample_ref.shape[0]
    arriving = pltpu.make_async_copy(sample_ref, left_ref, in_sem)
    arriving.start()
    share = count // (half // BLOCK)

    def low_half(start):
        if start == half:
            arriving.wait()
        if start >= half:
            rows = pl.ds((start - half) // BLOCK * share, share)
            low = dot(left_ref[rows, :half], inverse_ref[:half, :half], ((1,), (1,)))
            right_ref[rows, :half] = low * M**0.5

    invert_factor(sums_ref, inverse_ref, work_ref, low_half)
    leaving = []
    for index, start in enumerate(range(0, count, count // CHUNKS)):
        part = pl.ds(start, count // CHUNKS)
        high = dot(left_ref[part, :], inverse_ref[half:, :], ((1,), (1,)))
        right_ref[part, half:] = high * M**0.5
        leaving.append(
            pltpu.make_async_copy(right_ref.at[part], basis_ref.at[part], out_sems.at[index])
        )
        leaving[-1].start()
    products = sums_ref[half + half // 2 :, :]
    projection = dot(inverse_ref[...], products, ((1,), (1,)))
    mean = jnp.sum(projection * projection, axis=0, keepdims=True) / size
    coefficients_ref[...] = projection * lax.rsqrt(mean + 1e-06)
    for copy in leaving:
        copy.wait()


def work_for(rank):
    return pltpu.VMEM((rank, 2 * rank), jnp.float32)


def price_of(rank):
    return pl.CostEstimate(
        flops=2_000_000_000, transcendentals=rank, bytes_accessed=8 * rank * rank
    )


def inverse_factor(sums):
    rank = sums.shape[1]
    vmem = pl.BlockSpec(memory_space=pltpu.VMEM)
    return pl.pallas_call(
        invert_factor,
        out_shape=jax.ShapeDtypeStruct((rank, rank), jnp.float32),
        in_specs=[vmem],
        out_specs=vmem,
        scratch_shapes=[work_for(rank)],
        cost_estimate=price_of(rank),
        name="inverse_factor",
    )(sums)


def results(sums, sample, width):
    rank = sums.shape[1]
    vmem = pl.BlockSpec(memory_space=pltpu.VMEM)
    anywhere = pl.BlockSpec(memory_space=pl.ANY)
    return pl.pallas_call(
        result_kernel,
        out_shape=[
            jax.ShapeDtypeStruct(sample.shape, jnp.float32),
            jax.ShapeDtypeStruct((rank, width), jnp.float32),
        ],
        in_specs=[vmem, anywhere],
        out_specs=[anywhere, vmem],
        scratch_shapes=[
            pltpu.VMEM((rank, rank), jnp.float32),
            work_for(rank),
            pltpu.VMEM(sample.shape, jnp.float32),
            pltpu.VMEM(sample.shape, jnp.float32),
            pltpu.SemaphoreType.DMA(()),
            pltpu.SemaphoreType.DMA((CHUNKS,)),
        ],
        cost_estimate=price_of(rank),
        name="results",
    )(sums, sample)


def exchange(tiles, axis):
    return lax.all_to_all(tiles, axis, 0, 0, tiled=True)


def tiles_for(array, axis):
    return array.reshape(lax.axis_size(axis), -1, array.shape[-1])


def copies_for(array, axis):
    return jnp.broadcast_to(array[None], (lax.axis_size(axis), *array.shape))


def scatter_sum(array, axis):
    return exchange(tiles_for(array, axis), axis).sum(axis=0)


def gather(array, axis):
    return exchange(copies_for(array, axis), axis).reshape(-1, array.shape[-1])


def sum_over_rows(array):
    return gather(scatter_sum(array, ROWS), ROWS)


def sums_with(matrix, sample):
    half = sample.shape[1] // 2
    lower = dot(sample[:, half:], sample, ((0,), (0,)))
    corner = dot(sample[:, :half], sample[:, :half], ((0,), (0,)))
    corner = jnp.concatenate([corner[: half // 2], corner[half // 2 :]], axis=1)
    products = dot(matrix, sample, ((0,), (0,)))
    return sum_over_rows(jnp.concatenate([lower, corner, products], axis=0))


def per_device(matrix, sketch):
    width = matrix.shape[1]

    partial = dot(matrix, sketch, ((1,), (0,)))
    own = scatter_sum(scatter_sum(partial, NEAR), FAR)
    first = gather(gather(own, FAR), NEAR)

    sums = sums_with(matrix, first)
    inverse = inverse_factor(sums)
    partial = dot(matrix, sums[-width:], ((1,), (0,)))
    own = scatter_sum(scatter_sum(partial, NEAR), FAR)
    own = dot(own, inverse, ((1,), (1,)))
    second = gather(gather(own, FAR), NEAR)

    return tuple(results(sums_with(matrix, second), second, width))


def solution(mesh):
    columns, inner, outer = mesh.devices.shape
    split = Mesh(
        mesh.devices.reshape(4, columns // 8, 2, inner, outer),
        ("y", "z_high", "z_low", "inner", "outer"),
    )
    column = ("y", "z_high", "z_low")
    return jax.shard_map(
        per_device,
        mesh=split,
        in_specs=(P(ROWS, column), P(column, None)),
        out_specs=(P(ROWS, None), P(None, column)),
        check_vma=False,
    )
```
